32 devices in a mesh: dp: 2 (over x), kv: 4 (over z), tp: 4 (over y, core).
Axes of the slice: x: 2, y: 2, z: 4, core: 2. Of those that a mesh axis runs over, the one named last changes fastest.
Arguments:
- x: bfloat16 [16, 5120], P('dp'), parts along dimension 0
- ks_cache: bfloat16 [16, 8, 1024, 128], P('dp', 'tp', 'kv'), parts along dimension 0
- vs_cache: bfloat16 [16, 8, 1024, 128], P('dp', 'tp', 'kv'), parts along dimension 0
- seq_len: int32 [16], P('dp'), parts along dimension 0
- kx_cache: bfloat16 [16, 8, 6404, 128], P('dp', 'tp', 'kv'), parts along dimension 0
- vx_cache: bfloat16 [16, 8, 6404, 128], P('dp', 'tp', 'kv'), parts along dimension 0
- tile_vis: int32 [16, 4], P('dp'), parts along dimension 0
- attn_norm: bfloat16 [5120], replicated
- wq_self: bfloat16 [5120, 5120], P(None, 'tp')
- wk_self: bfloat16 [5120, 1024], P(None, 'tp')
- wv_self: bfloat16 [5120, 1024], P(None, 'tp')
- wo_self: bfloat16 [5120, 5120], P('tp')
- mlp_norm: bfloat16 [5120], replicated
- wg_self: bfloat16 [5120, 13824], P(None, 'tp')
- wu_self: bfloat16 [5120, 13824], P(None, 'tp')
- wd_self: bfloat16 [13824, 5120], P('tp')
- xattn_norm: bfloat16 [5120], replicated
- wq_cross: bfloat16 [5120, 5120], P(None, 'tp')
- q_norm: bfloat16 [128], replicated
- wo_cross: bfloat16 [5120, 5120], P('tp')
- cross_gates: float32 [2], replicated
- xmlp_norm: bfloat16 [5120], replicated
- wg_cross: bfloat16 [5120, 13824], P(None, 'tp')
- wu_cross: bfloat16 [5120, 13824], P(None, 'tp')
- wd_cross: bfloat16 [13824, 5120], P('tp')
Outputs:
- output 1: bfloat16 [16, 5120], P('dp'), parts along dimension 0
- output 2: bfloat16 [16, 8, 128], P('dp', 'tp'), parts along dimension 0
- output 3: bfloat16 [16, 8, 128], P('dp', 'tp'), parts along dimension 0
There are 2 independent parts. The reference program is written for one: setup_inputs(seed, part) draws one part's arguments, and reference() takes and returns one part's arrays. A program takes and returns all parts, laid end to end along the dimension named above; an argument that names none is the same for every part.
All inputs are finite; a program needn't handle non-finite values.
Results may differ from the reference program's by a relative error of at most 0.0130243.
Values sent between devices are 32-bit elements.
A program may use at most 1.25 GiB of HBM per device.

```python
import math
import jax
import jax.numpy as jnp
from jax import lax

D = 5120
HEADS = 40
KV_HEADS = 8
HEAD = 128
FF = 13824
TILES = 4
TILE_TOK = 1601
BATCH = 8
CACHE_LEN = 1024
NORM_EPS = 1e-5
ROPE_THETA = 500000.0
MASK_VALUE = -1e30


def rope_freqs():
    freq_list = []
    for index in range(HEAD // 2):
        base_freq = 1.0 / (ROPE_THETA ** (2.0 * index / HEAD))
        wave_len = 2.0 * math.pi / base_freq
        if wave_len < 2048.0:
            freq_list.append(base_freq)
        elif wave_len > 8192.0:
            freq_list.append(base_freq / 8.0)
        else:
            smooth = (8192.0 / wave_len - 1.0) / 3.0
            freq_list.append((1.0 - smooth) * base_freq / 8.0 + smooth * base_freq)
    return jnp.array(freq_list, dtype=jnp.float32)


def rms_norm(hidden, gain):
    return hidden * lax.rsqrt(jnp.mean(hidden * hidden, axis=-1, keepdims=True) + NORM_EPS) * gain.astype(jnp.float32)


def apply_rope(tensor, cos_t, sin_t):
    half = tensor.shape[-1] // 2
    first = tensor[..., :half]
    second = tensor[..., half:]
    return jnp.concatenate([first * cos_t - second * sin_t, second * cos_t + first * sin_t], axis=-1)


def swiglu(hidden, gain, w_gate, w_up, w_down):
    h_norm = rms_norm(hidden, gain).astype(jnp.bfloat16)
    gate = jnp.dot(h_norm, w_gate, preferred_element_type=jnp.float32)
    upper = jnp.dot(h_norm, w_up, preferred_element_type=jnp.float32)
    hidden_act = (jax.nn.silu(gate) * upper).astype(jnp.bfloat16)
    return jnp.dot(hidden_act, w_down, preferred_element_type=jnp.float32)


def attend_row(query, keys, values, visible):
    scores = jnp.einsum('kgd,ktd->kgt', query.astype(jnp.float32), keys.astype(jnp.float32)) * HEAD ** -0.5
    scores = jnp.where(visible[None, None, :], scores, MASK_VALUE)
    top = jnp.max(scores, axis=-1, keepdims=True)
    weights = jnp.where(visible[None, None, :], jnp.exp(scores - top), 0.0)
    total = jnp.sum(weights, axis=-1, keepdims=True)
    out = jnp.einsum('kgt,ktd->kgd', weights, values.astype(jnp.float32))
    return (out / jnp.where(total > 0, total, 1.0)).reshape(-1).astype(jnp.bfloat16)


def setup_inputs(seed: int = 0, part: int = 0) -> dict:
    wkeys = jax.random.split(jax.random.key(seed), 20)
    pkeys = jax.random.split(jax.random.fold_in(jax.random.key(seed + 1), part), 16)

    def draw_matrix(key, rows, cols, factor=1.0):
        return (jax.random.normal(key, (rows, cols), jnp.float32) * (factor * rows ** -0.5)).astype(jnp.bfloat16)

    def draw_gain(key, size, spread):
        return (1.0 + spread * jax.random.normal(key, (size,), jnp.float32)).astype(jnp.bfloat16)

    blocks = 8
    x = jax.random.normal(pkeys[0], (BATCH, D), jnp.float32).astype(jnp.bfloat16)
    coarse_k = jax.random.normal(pkeys[1], (BATCH, KV_HEADS, blocks, 1, HEAD), jnp.float32)
    noise_k = jax.random.normal(pkeys[2], (BATCH, KV_HEADS, blocks, CACHE_LEN // blocks, HEAD), jnp.float32)
    ks_cache = (noise_k + coarse_k).reshape(BATCH, KV_HEADS, CACHE_LEN, HEAD).astype(jnp.bfloat16)
    coarse_v = jax.random.normal(pkeys[3], (BATCH, KV_HEADS, blocks, 1, HEAD), jnp.float32)
    noise_v = jax.random.normal(pkeys[4], (BATCH, KV_HEADS, blocks, CACHE_LEN // blocks, HEAD), jnp.float32)
    vs_cache = (0.6 * noise_v + coarse_v).reshape(BATCH, KV_HEADS, CACHE_LEN, HEAD).astype(jnp.bfloat16)
    tile_k = jax.random.normal(pkeys[5], (BATCH, KV_HEADS, TILES, 1, HEAD), jnp.float32)
    noise_kx = jax.random.normal(pkeys[6], (BATCH, KV_HEADS, TILES, TILE_TOK, HEAD), jnp.float32)
    kx_cache = (noise_kx + tile_k).reshape(BATCH, KV_HEADS, TILES * TILE_TOK, HEAD).astype(jnp.bfloat16)
    tile_v = jax.random.normal(pkeys[7], (BATCH, KV_HEADS, TILES, 1, HEAD), jnp.float32)
    noise_vx = jax.random.normal(pkeys[8], (BATCH, KV_HEADS, TILES, TILE_TOK, HEAD), jnp.float32)
    vx_cache = (0.6 * noise_vx + tile_v).reshape(BATCH, KV_HEADS, TILES * TILE_TOK, HEAD).astype(jnp.bfloat16)
    row_ids = jnp.arange(BATCH)
    kind = jax.random.randint(pkeys[9], (BATCH,), 0, 4)
    short_len = jax.random.randint(pkeys[10], (BATCH,), 0, 8)
    long_len = jax.random.randint(pkeys[11], (BATCH,), 0, CACHE_LEN)
    seq_len = jnp.where(row_ids == 0, CACHE_LEN - 1, jnp.where(kind == 0, short_len, long_len)).astype(jnp.int32)
    cols = jnp.arange(TILES)[None, :]
    forced = (cols == (row_ids % TILES)[:, None]) | (cols == ((row_ids + TILES // 2) % TILES)[:, None])
    coin = jax.random.randint(pkeys[12], (BATCH, TILES), 0, 2)
    dropped = (jax.random.randint(pkeys[13], (BATCH,), 0, 4) == 0) & (row_ids > 0)
    tile_vis = jnp.where(dropped[:, None], 0, jnp.where(forced, 1, coin)).astype(jnp.int32)
    gate_raw = jax.random.uniform(wkeys[16], (2,), jnp.float32, -1.0, 1.0)
    cross_gates = jnp.where(gate_raw < 0, -1.0, 1.0) * (0.3 + 1.7 * jnp.abs(gate_raw))
    return {
        'x': x,
        'ks_cache': ks_cache,
        'vs_cache': vs_cache,
        'seq_len': seq_len,
        'kx_cache': kx_cache,
        'vx_cache': vx_cache,
        'tile_vis': tile_vis,
        'attn_norm': draw_gain(wkeys[0], D, 0.35),
        'wq_self': draw_matrix(wkeys[1], D, HEADS * HEAD),
        'wk_self': draw_matrix(wkeys[2], D, KV_HEADS * HEAD),
        'wv_self': draw_matrix(wkeys[3], D, KV_HEADS * HEAD),
        'wo_self': draw_matrix(wkeys[4], HEADS * HEAD, D),
        'mlp_norm': draw_gain(wkeys[5], D, 0.2),
        'wg_self': draw_matrix(wkeys[6], D, FF),
        'wu_self': draw_matrix(wkeys[7], D, FF),
        'wd_self': draw_matrix(wkeys[8], FF, D),
        'xattn_norm': draw_gain(wkeys[9], D, 0.2),
        'wq_cross': draw_matrix(wkeys[10], D, HEADS * HEAD),
        'q_norm': draw_gain(wkeys[11], HEAD, 0.5),
        'wo_cross': draw_matrix(wkeys[12], HEADS * HEAD, D, factor=1.5),
        'cross_gates': cross_gates,
        'xmlp_norm': draw_gain(wkeys[13], D, 0.2),
        'wg_cross': draw_matrix(wkeys[14], D, FF),
        'wu_cross': draw_matrix(wkeys[15], D, FF),
        'wd_cross': draw_matrix(wkeys[17], FF, D, factor=1.5),
    }


def reference(x, ks_cache, vs_cache, seq_len, kx_cache, vx_cache, tile_vis, attn_norm, wq_self, wk_self, wv_self, wo_self, mlp_norm, wg_self, wu_self, wd_self, xattn_norm, wq_cross, q_norm, wo_cross, cross_gates, xmlp_norm, wg_cross, wu_cross, wd_cross):
    group = HEADS // KV_HEADS
    x_float = x.astype(jnp.float32)
    angles = seq_len.astype(jnp.float32)[:, None] * rope_freqs()[None, :]
    cos_t = jnp.cos(angles)[:, None, :]
    sin_t = jnp.sin(angles)[:, None, :]
    x_norm = rms_norm(x_float, attn_norm).astype(jnp.bfloat16)
    query = apply_rope(jnp.dot(x_norm, wq_self, preferred_element_type=jnp.float32).reshape(BATCH, HEADS, HEAD), cos_t, sin_t)
    query = query.astype(jnp.bfloat16).reshape(BATCH, KV_HEADS, group, HEAD)
    key_new = apply_rope(jnp.dot(x_norm, wk_self, preferred_element_type=jnp.float32).reshape(BATCH, KV_HEADS, HEAD), cos_t, sin_t).astype(jnp.bfloat16)
    val_new = jnp.dot(x_norm, wv_self, preferred_element_type=jnp.float32).astype(jnp.bfloat16).reshape(BATCH, KV_HEADS, HEAD)
    slot_ids = jnp.arange(CACHE_LEN)[None, :]
    slot_hit = (slot_ids == seq_len[:, None])[:, None, :, None]
    keys_full = jnp.where(slot_hit, key_new[:, :, None, :], ks_cache)
    values_full = jnp.where(slot_hit, val_new[:, :, None, :], vs_cache)
    visible_self = slot_ids <= seq_len[:, None]
    attn_self = lax.map(lambda row: attend_row(row[0], row[1], row[2], row[3]), (query, keys_full, values_full, visible_self))
    h_one = (x_float + jnp.dot(attn_self, wo_self, preferred_element_type=jnp.float32)).astype(jnp.bfloat16)
    h_one_f = h_one.astype(jnp.float32)
    h_two = (h_one_f + swiglu(h_one_f, mlp_norm, wg_self, wu_self, wd_self)).astype(jnp.bfloat16)
    h_two_f = h_two.astype(jnp.float32)
    cx_norm = rms_norm(h_two_f, xattn_norm).astype(jnp.bfloat16)
    query_x = jnp.dot(cx_norm, wq_cross, preferred_element_type=jnp.float32).reshape(BATCH, HEADS, HEAD)
    query_x = rms_norm(query_x, q_norm).astype(jnp.bfloat16).reshape(BATCH, KV_HEADS, group, HEAD)
    tile_on = tile_vis != 0
    visible_cross = jnp.broadcast_to(tile_on[:, :, None], (BATCH, TILES, TILE_TOK)).reshape(BATCH, TILES * TILE_TOK)
    attn_cross = lax.map(lambda row: attend_row(row[0], row[1], row[2], row[3]), (query_x, kx_cache, vx_cache, visible_cross))
    row_on = jnp.any(tile_on, axis=1).astype(jnp.float32)[:, None]
    gates = jnp.tanh(cross_gates)
    h_three = (h_two_f + gates[0] * row_on * jnp.dot(attn_cross, wo_cross, preferred_element_type=jnp.float32)).astype(jnp.bfloat16)
    h_three_f = h_three.astype(jnp.float32)
    h_four = (h_three_f + gates[1] * row_on * swiglu(h_three_f, xmlp_norm, wg_cross, wu_cross, wd_cross)).astype(jnp.bfloat16)
    return (h_four, key_new, val_new)
```

```python
import functools
import math
import numpy as np
import jax
import jax.numpy as jnp
from jax import lax
from jax.experimental import pallas as pl
from jax.experimental.pallas import tpu as pltpu
from jax.sharding import PartitionSpec as P

NORM_EPS = 1e-5
ROPE_THETA = 500000.0
MASK_VALUE = -1e30
MESH = pl.DeviceIdType.MESH
BF16 = jnp.bfloat16
F32 = jnp.float32

BATCH = 8
HEAD = 128
HEADS = 10
GROUPS = 2
PER = HEADS // GROUPS
HID = 5120
BLK = 1280
QW = HEADS * HEAD
KVW = GROUPS * HEAD
FFW = 896
FF_TILES = 27
SLOTS = 256
TOK = 1601
VMEM_LIMIT = 67043328
PIECE = 640
SCALE = HEAD ** -0.5
N_LOCAL = 64
N_REMOTE = 48


def rope_freqs(head_dim):
    freq_list = []
    for index in range(head_dim // 2):
        base_freq = 1.0 / (ROPE_THETA ** (2.0 * index / head_dim))
        wave_len = 2.0 * math.pi / base_freq
        if wave_len < 2048.0:
            freq_list.append(base_freq)
        elif wave_len > 8192.0:
            freq_list.append(base_freq / 8.0)
        else:
            smooth = (8192.0 / wave_len - 1.0) / 3.0
            freq_list.append((1.0 - smooth) * base_freq / 8.0 + smooth * base_freq)
    return np.array(freq_list + freq_list, dtype=np.float32)


def dot(a, b):
    return jnp.dot(a, b, preferred_element_type=F32)


def bf(value):
    return value.astype(BF16).astype(F32)


def kernel(x_h, gains_h, rope_h, gates_ref, seq_ref, vis_h,
           ks_h, vs_h, kx_h, vx_h,
           wq1_h, wk_h, wv_h, wo1_h, wg1_h, wu1_h, wd1_h,
           wq2_h, wo2_h, wg2_h, wu2_h, wd2_h,
           h_out, k_out, v_out,
           x_v, gains_v, rope_v, vis_v, buf_a, buf_o,
           u_v, qbd_v, o_v, s_self, p_self, s_cross, p_cross,
           comb, part, rs_buf, hs_buf, y_buf, zs_buf, zr_buf, t_buf, ty_buf, hbuf,
           lsem, wsem, send_sem, recv_sem):
    tp = lax.axis_index("tp")
    kv = lax.axis_index("kv")
    core = lax.rem(tp, 2)
    mate_tp = tp + 1 - 2 * core
    mate = {"tp": mate_tp}
    across = {"tp": lax.rem(tp + 2, 4)}
    around = [lax.rem(kv + j, 4) for j in (3, 2, 1)]
    counts = {"remote": 0, "local": 0}

    def remote(src, dst, device):
        i = counts["remote"]
        counts["remote"] += 1
        copy = pltpu.make_async_remote_copy(src_ref=src, dst_ref=dst, send_sem=send_sem.at[i],
                                            recv_sem=recv_sem.at[i], device_id=device, device_id_type=MESH)
        copy.start()
        return copy

    def local(src, dst):
        i = counts["local"]
        counts["local"] += 1
        copy = pltpu.make_async_copy(src, dst, lsem.at[i])
        copy.start()
        return copy

    def wait_all(copies):
        for copy in copies:
            copy.wait()

    ff_off = pl.multiple_of(jnp.minimum(kv * 7, FF_TILES - 7) * 128, 128)

    def copy_a(w_h, c):
        return pltpu.make_async_copy(w_h.at[pl.ds(c * BLK, BLK), :], buf_a.at[c], wsem.at[c])

    def copies_a(w_h):
        return [copy_a(w_h, c) for c in range(4)]

    def copies_o(w_h):
        return [pltpu.make_async_copy(w_h.at[:, pl.ds(c * BLK, BLK)], buf_o.at[c], wsem.at[4 + c]) for c in range(4)]

    def copies_up(wg_h, wu_h, gu):
        return [pltpu.make_async_copy(w_h.at[pl.ds(c * BLK, BLK), pl.ds(ff_off, FFW)], gu.at[c, :, pl.ds(i * FFW, FFW)],
                                      wsem.at[8 + 2 * c + i]) for c in range(4) for i, w_h in enumerate((wg_h, wu_h))]

    def copies_down(wd_h, dn):
        return [pltpu.make_async_copy(wd_h.at[pl.ds(ff_off, FFW), pl.ds(c * BLK, BLK)], dn.at[c], wsem.at[16 + c])
                for c in range(4)]

    def start_all(copies):
        for copy in copies:
            copy.start()

    first = [local(x_h, x_v), local(gains_h, gains_v), local(rope_h, rope_v), local(vis_h, vis_v)]
    rows = lax.broadcasted_iota(jnp.int32, (BATCH, 1), 0)
    lanes = lax.broadcasted_iota(jnp.int32, (BATCH, HEAD), 1)
    seq = jnp.zeros((BATCH, 1), jnp.int32)
    for b in range(BATCH):
        seq = jnp.where(rows == b, seq_ref[b], seq)

    def norm_to_u(slot, gain_row):
        total = jnp.zeros((BATCH, 1), F32)
        for p in range(8):
            h = hbuf[slot, p]
            total = total + jnp.sum(h * h, axis=-1, keepdims=True)
        scale = lax.rsqrt(total / HID + NORM_EPS)
        for p in range(8):
            u_v[p] = hbuf[slot, p] * scale * gains_v[gain_row:gain_row + 1, p * PIECE:(p + 1) * PIECE]

    def u_block(c):
        return jnp.concatenate([u_v[2 * c], u_v[2 * c + 1]], axis=-1).astype(BF16)

    def put_queries(query):
        zero = jnp.zeros((BATCH, HEAD), F32)
        for r in range(HEADS):
            g = r // PER
            qbd_v[r * BATCH:(r + 1) * BATCH, g * HEAD:(g + 1) * HEAD] = query[r]
            qbd_v[r * BATCH:(r + 1) * BATCH, (1 - g) * HEAD:(2 - g) * HEAD] = zero

    def scores(keys, s_ref):
        q = qbd_v[...].astype(BF16)
        for b in range(BATCH):
            k_cat = jnp.concatenate([keys[b, 0], keys[b, 1]], axis=-1)
            s = lax.dot_general(q, k_cat, (((1,), (1,)), ((), ())), preferred_element_type=F32)
            for r in range(HEADS):
                s_ref[r, b:b + 1, :] = s[r * BATCH + b:r * BATCH + b + 1, :]

    def weigh(values, p_ref):
        for b in range(BATCH):
            v_cat = jnp.concatenate([values[b, 0], values[b, 1]], axis=-1)
            o = dot(p_ref[...], v_cat)
            for r in range(HEADS):
                g = r // PER
                o_v[r, b:b + 1, :] = o[r * BATCH + b:r * BATCH + b + 1, g * HEAD:(g + 1) * HEAD]

    def put_partials(slot, outs, tops, totals):
        top_row = jnp.full((BATCH, HEAD), MASK_VALUE, F32)
        total_row = jnp.zeros((BATCH, HEAD), F32)
        for r in range(HEADS):
            comb[slot, kv, :, r * HEAD:(r + 1) * HEAD] = outs[r]
            top_row = jnp.where(lanes == r, tops[r], top_row)
            total_row = jnp.where(lanes == r, totals[r], total_row)
        comb[slot, kv, :, QW:QW + HEAD] = top_row
        comb[slot, kv, :, QW + HEAD:QW + 2 * HEAD] = total_row

    def exchange_partials(slot):
        wait_all([remote(comb.at[slot, kv], comb.at[slot, kv], {"kv": peer}) for peer in around])
        best = comb[slot, 0, :, QW:QW + HEAD]
        for s in range(1, 4):
            best = jnp.maximum(best, comb[slot, s, :, QW:QW + HEAD])
        weight = [jnp.exp(comb[slot, s, :, QW:QW + HEAD] - best) for s in range(4)]
        norm = sum(comb[slot, s, :, QW + HEAD:QW + 2 * HEAD] * weight[s] for s in range(4))
        inverse = 1.0 / jnp.where(norm > 0, norm, 1.0)
        heads = []
        for r in range(HEADS):
            mixed = sum(comb[slot, s, :, r * HEAD:(r + 1) * HEAD] * weight[s][:, r:r + 1] for s in range(4))
            heads.append(mixed * inverse[:, r:r + 1])
        return jnp.concatenate(heads, axis=-1).astype(BF16)

    def halves(slot, left, w_ref):
        def run(base):
            def body(i, carry):
                out = dot(left, w_ref[base + i])
                part[slot, 2 * (base + i)] = out[:, :PIECE]
                part[slot, 2 * (base + i) + 1] = out[:, PIECE:]
                return carry
            lax.fori_loop(0, 2, body, 0)
        run(2 * (1 - core))
        copy = remote(part.at[slot, pl.ds(4 * (1 - core), 4)], rs_buf.at[slot], mate)
        run(2 * core)
        copy.wait()

    def reduce_plane(slot, i_h, h_from, h_to, finish):
        sends = []
        for i in range(2):
            for j in (2 * i, 2 * i + 1):
                hs_buf[i_h, j] = part[slot, 4 * core + j] + rs_buf[slot, j]
            sends.append(remote(hs_buf.at[i_h, pl.ds(2 * i, 2)], y_buf.at[i_h, pl.ds(2 * i, 2)], across))
        backs = []
        for i in range(2):
            sends[i].wait()
            for j in (2 * i, 2 * i + 1):
                p = 4 * core + j
                hbuf[h_to, p] = bf(finish(hbuf[h_from, p], hs_buf[i_h, j] + y_buf[i_h, j]))
            span = hbuf.at[h_to, pl.ds(4 * core + 2 * i, 2)]
            backs.append(remote(span, span, mate))
        wait_all(backs)

    def reduce_all(slot, i_z, h_from, h_to, finish):
        for j in range(4):
            zs_buf[i_z, j] = part[slot, 4 * core + j] + rs_buf[slot, j]
        copies = [remote(zs_buf.at[i_z, peer], zr_buf.at[i_z, kv], {"kv": peer}) for peer in around]
        zr_buf[i_z, kv] = zs_buf[i_z, kv]
        wait_all(copies)
        t_buf[i_z] = zr_buf[i_z, 0] + zr_buf[i_z, 1] + zr_buf[i_z, 2] + zr_buf[i_z, 3]
        remote(t_buf.at[i_z], ty_buf.at[i_z], across).wait()
        p = 4 * core + kv
        hbuf[h_to, p] = bf(finish(hbuf[h_from, p], t_buf[i_z] + ty_buf[i_z]))
        own = hbuf.at[h_to, p]
        copies = []
        for peer in around:
            copies.append(remote(own, own, {"kv": peer}))
            copies.append(remote(own, own, {"kv": peer, "tp": mate_tp}))
        copies.append(remote(own, own, mate))
        wait_all(copies)

    def mlp(slot, gain_row, h_slot, gu, dn, up, down):
        norm_to_u(h_slot, gain_row)
        acc = jnp.zeros((BATCH, 2 * FFW), F32)
        for c in range(4):
            wait_all(up[2 * c:2 * c + 2])
            acc = acc + dot(u_block(c), gu[c])
        gate, upper = acc[:, :FFW], acc[:, FFW:]
        act = gate * (1.0 / (1.0 + jnp.exp(-gate))) * upper
        keep = jnp.logical_or(kv < 3, lax.broadcasted_iota(jnp.int32, (BATCH, FFW), 1) >= 128)
        act = jnp.where(keep, act, 0.0).astype(BF16)
        wait_all(down)
        halves(slot, act, dn)

    start_all(copies_a(wq1_h))

    def self_attention(wkv, ks, vs, gu):
        w_kv = [(local(wk_h.at[pl.ds(c * BLK, BLK), :], wkv.at[c, :, pl.ds(0, KVW)]),
                 local(wv_h.at[pl.ds(c * BLK, BLK), :], wkv.at[c, :, pl.ds(KVW, KVW)])) for c in range(4)]
        caches = [local(ks_h, ks), local(vs_h, vs)]
        start_all(copies_o(wo1_h))
        start_all(copies_up(wg1_h, wu1_h, gu))

        barrier = pltpu.get_barrier_semaphore()
        peers = [{"kv": peer} for peer in around] + [{"kv": peer, "tp": mate_tp} for peer in around] + [mate, across]
        for peer in peers:
            pl.semaphore_signal(barrier, inc=1, device_id=peer, device_id_type=MESH)

        wait_all(first)
        for p in range(8):
            hbuf[0, p] = x_v[:, p * PIECE:(p + 1) * PIECE].astype(F32)
        norm_to_u(0, 0)
        angles = seq.astype(F32) * rope_v[0:1, :]
        cos_t = jnp.cos(angles)
        sin_t = jnp.sin(angles) * jnp.where(lanes < HEAD // 2, -1.0, 1.0)

        def rope(z):
            return bf(z * cos_t + pltpu.roll(z, HEAD // 2, 1) * sin_t)

        acc_q = jnp.zeros((BATCH, QW), F32)
        acc_kv = jnp.zeros((BATCH, 2 * KVW), F32)
        for c in range(4):
            copy_a(wq1_h, c).wait()
            wait_all(w_kv[c])
            left = u_block(c)
            acc_q = acc_q + dot(left, buf_a[c])
            acc_kv = acc_kv + dot(left, wkv[c])
        query = [rope(acc_q[:, r * HEAD:(r + 1) * HEAD]) for r in range(HEADS)]
        key_new = [rope(acc_kv[:, g * HEAD:(g + 1) * HEAD]) for g in range(GROUPS)]
        val_new = [bf(acc_kv[:, KVW + g * HEAD:KVW + (g + 1) * HEAD]) for g in range(GROUPS)]
        for g in range(GROUPS):
            k_out[:, g * HEAD:(g + 1) * HEAD] = key_new[g].astype(BF16)
            v_out[:, g * HEAD:(g + 1) * HEAD] = val_new[g].astype(BF16)
        put_queries(query)
        wait_all(caches)
        scores(ks, s_self)
        slot_ids = kv * SLOTS + lax.broadcasted_iota(jnp.int32, (BATCH, SLOTS), 1)
        visible = slot_ids < seq
        owner = jnp.logical_and(seq >= kv * SLOTS, seq < (kv + 1) * SLOTS)
        tops, totals, news = [], [], []
        for pair in range(HEADS // 2):
            both = []
            for r in (2 * pair, 2 * pair + 1):
                s = jnp.where(visible, s_self[r] * SCALE, MASK_VALUE)
                new = jnp.sum(query[r] * key_new[r // PER], axis=-1, keepdims=True) * SCALE
                new = jnp.where(owner, new, MASK_VALUE)
                top = jnp.maximum(jnp.max(s, axis=-1, keepdims=True), new)
                prob = jnp.where(visible, jnp.exp(s - top), 0.0)
                new_prob = jnp.where(owner, jnp.exp(new - top), 0.0)
                tops.append(top)
                totals.append(jnp.sum(prob, axis=-1, keepdims=True) + new_prob)
                news.append(new_prob)
                both.append(prob)
            p_self[2 * pair * BATCH:(2 * pair + 2) * BATCH, :] = jnp.concatenate(both, axis=0).astype(BF16)
        weigh(vs, p_self)
        outs = [o_v[r] + news[r] * val_new[r // PER] for r in range(HEADS)]
        pl.semaphore_wait(barrier, len(peers))
        put_partials(0, outs, tops, totals)

    def self_rest(dn, gu):
        start_all(copies_down(wd1_h, dn))
        start_all(copies_a(wq2_h))
        attn = exchange_partials(0)
        wait_all(copies_o(wo1_h))
        halves(0, attn, buf_o)
        start_all(copies_o(wo2_h))
        reduce_plane(0, 0, 0, 1, lambda h, s: h + s)
        mlp(1, 1, 1, gu, dn, copies_up(wg1_h, wu1_h, gu), copies_down(wd1_h, dn))

    up_space = pltpu.VMEM((4, BLK, 2 * FFW), BF16)
    down_space = pltpu.VMEM((4, FFW, BLK), BF16)

    def phase_one(gu):
        pl.run_scoped(functools.partial(self_attention, gu=gu), pltpu.VMEM((4, BLK, 2 * KVW), BF16),
                      pltpu.VMEM((BATCH, GROUPS, SLOTS, HEAD), BF16), pltpu.VMEM((BATCH, GROUPS, SLOTS, HEAD), BF16))
        pl.run_scoped(functools.partial(self_rest, gu=gu), down_space)

    pl.run_scoped(phase_one, up_space)

    visible_tile = jnp.sum(jnp.where(lax.broadcasted_iota(jnp.int32, (BATCH, 4), 1) == kv, vis_v[...], 0),
                           axis=-1, keepdims=True) > 0
    row_on = jnp.where(jnp.sum(vis_v[...], axis=-1, keepdims=True) > 0, 1.0, 0.0)

    def scope_two(kx, vx):
        caches = [local(kx_h, kx), local(vx_h, vx)]
        reduce_all(1, 0, 1, 2, lambda h, s: h + s)
        norm_to_u(2, 2)
        acc = jnp.zeros((BATCH, QW), F32)
        for c in range(4):
            copy_a(wq2_h, c).wait()
            acc = acc + dot(u_block(c), buf_a[c])
        query = []
        for r in range(HEADS):
            z = acc[:, r * HEAD:(r + 1) * HEAD]
            z = z * lax.rsqrt(jnp.mean(z * z, axis=-1, keepdims=True) + NORM_EPS) * gains_v[4:5, 0:HEAD]
            query.append(bf(z))
        put_queries(query)
        wait_all(caches)
        scores(kx, s_cross)
        tops, totals = [], []
        for pair in range(HEADS // 2):
            both = []
            for r in (2 * pair, 2 * pair + 1):
                s = s_cross[r] * SCALE
                top = jnp.max(s, axis=-1, keepdims=True)
                prob = jnp.exp(s - top)
                tops.append(jnp.where(visible_tile, top, MASK_VALUE))
                totals.append(jnp.where(visible_tile, jnp.sum(prob, axis=-1, keepdims=True), 0.0))
                both.append(prob)
            p_cross[2 * pair * BATCH:(2 * pair + 2) * BATCH, :] = jnp.concatenate(both, axis=0).astype(BF16)
        weigh(vx, p_cross)
        outs = [jnp.where(visible_tile, o_v[r], 0.0) for r in range(HEADS)]
        put_partials(1, outs, tops, totals)

    pl.run_scoped(scope_two, pltpu.VMEM((BATCH, GROUPS, TOK, HEAD), BF16), pltpu.VMEM((BATCH, GROUPS, TOK, HEAD), BF16))

    def gate(i):
        return jnp.tanh(jnp.full((BATCH, HEAD), gates_ref[i], F32))[:, 0:1] * row_on

    def scope_three(gu, dn):
        start_all(copies_up(wg2_h, wu2_h, gu))
        start_all(copies_down(wd2_h, dn))
        attn = exchange_partials(1)
        wait_all(copies_o(wo2_h))
        halves(2, attn, buf_o)
        reduce_plane(2, 1, 2, 3, lambda h, s: h + gate(0) * s)
        mlp(3, 3, 3, gu, dn, copies_up(wg2_h, wu2_h, gu), copies_down(wd2_h, dn))

    pl.run_scoped(scope_three, up_space, down_space)
    reduce_all(3, 1, 3, 4, lambda h, s: h + gate(1) * s)
    for p in range(8):
        h_out[:, p * PIECE:(p + 1) * PIECE] = hbuf[4, p].astype(BF16)


def solution(mesh):
    rows_spec = P('dp', None)
    cache_spec = P('dp', 'tp', 'kv', None)
    new_spec = P('dp', 'tp', None)
    col_spec = P(None, 'tp')
    row_spec = P('tp', None)
    vec_spec = P(None)
    in_specs = (rows_spec, cache_spec, cache_spec, P('dp'), cache_spec, cache_spec, rows_spec,
                vec_spec, col_spec, col_spec, col_spec, row_spec, vec_spec, col_spec, col_spec, row_spec,
                vec_spec, col_spec, vec_spec, row_spec, vec_spec, vec_spec, col_spec, col_spec, row_spec)
    out_specs = (rows_spec, new_spec, new_spec)

    def device_step(x, ks_cache, vs_cache, seq_len, kx_cache, vx_cache, tile_vis, attn_norm, wq_self, wk_self, wv_self, wo_self, mlp_norm, wg_self, wu_self, wd_self, xattn_norm, wq_cross, q_norm, wo_cross, cross_gates, xmlp_norm, wg_cross, wu_cross, wd_cross):
        gains = jnp.stack([attn_norm, mlp_norm, xattn_norm, xmlp_norm, jnp.pad(q_norm, (0, HID - HEAD))]
                          + [jnp.zeros_like(attn_norm)] * 3).astype(F32)
        freqs = jnp.tile(jnp.asarray(rope_freqs(HEAD))[None, :], (8, 1))
        hbm = pl.BlockSpec(memory_space=pl.ANY)
        smem = pl.BlockSpec(memory_space=pltpu.SMEM)
        vmem = pl.BlockSpec(memory_space=pltpu.VMEM)
        piece = (8, BATCH, PIECE)
        scratch = [
            pltpu.VMEM((BATCH, HID), BF16), pltpu.VMEM((8, HID), F32), pltpu.VMEM((8, HEAD), F32), pltpu.VMEM((BATCH, 4), jnp.int32),
            pltpu.VMEM((4, BLK, BLK), BF16), pltpu.VMEM((4, BLK, BLK), BF16),
            pltpu.VMEM(piece, F32), pltpu.VMEM((HEADS * BATCH, 2 * HEAD), F32), pltpu.VMEM((HEADS, BATCH, HEAD), F32),
            pltpu.VMEM((HEADS, BATCH, SLOTS), F32), pltpu.VMEM((HEADS * BATCH, SLOTS), BF16),
            pltpu.VMEM((HEADS, BATCH, TOK), F32), pltpu.VMEM((HEADS * BATCH, TOK), BF16),
            pltpu.VMEM((2, 4, BATCH, QW + 2 * HEAD), F32),
            pltpu.VMEM((4,) + piece, F32), pltpu.VMEM((4, 4, BATCH, PIECE), F32),
            pltpu.VMEM((2, 4, BATCH, PIECE), F32), pltpu.VMEM((2, 4, BATCH, PIECE), F32),
            pltpu.VMEM((2, 4, BATCH, PIECE), F32), pltpu.VMEM((2, 4, BATCH, PIECE), F32),
            pltpu.VMEM((2, BATCH, PIECE), F32), pltpu.VMEM((2, BATCH, PIECE), F32),
            pltpu.VMEM((5,) + piece, F32),
            pltpu.SemaphoreType.DMA((N_LOCAL,)), pltpu.SemaphoreType.DMA((20,)), pltpu.SemaphoreType.DMA((N_REMOTE,)), pltpu.SemaphoreType.DMA((N_REMOTE,)),
        ]
        h, key_new, val_new = pl.pallas_call(
            kernel,
            out_shape=(jax.ShapeDtypeStruct((BATCH, HID), BF16), jax.ShapeDtypeStruct((BATCH, KVW), BF16),
                       jax.ShapeDtypeStruct((BATCH, KVW), BF16)),
            in_specs=[hbm, hbm, hbm, smem, smem, hbm] + [hbm] * 16,
            out_specs=(vmem, vmem, vmem),
            scratch_shapes=scratch,
            compiler_params=pltpu.CompilerParams(collective_id=0, has_side_effects=True, vmem_limit_bytes=VMEM_LIMIT),
        )(x, gains, freqs, cross_gates, seq_len, tile_vis, ks_cache, vs_cache, kx_cache, vx_cache,
          wq_self, wk_self, wv_self, wo_self, wg_self, wu_self, wd_self, wq_cross, wo_cross, wg_cross, wu_cross, wd_cross)
        return h, key_new.reshape(BATCH, GROUPS, HEAD), val_new.reshape(BATCH, GROUPS, HEAD)

    return jax.shard_map(device_step, mesh=mesh, in_specs=in_specs, out_specs=out_specs, check_vma=False)
```

```python
import functools
import math
import numpy as np
import jax
import jax.numpy as jnp
from jax import lax
from jax.experimental import pallas as pl
from jax.experimental.pallas import tpu as pltpu
from jax.sharding import PartitionSpec as P

NORM_EPS = 1e-5
ROPE_THETA = 500000.0
MASK_VALUE = -1e30
MESH = pl.DeviceIdType.MESH
BF16 = jnp.bfloat16
F32 = jnp.float32

BATCH = 8
HEAD = 128
HEADS = 10
GROUPS = 2
PER = HEADS // GROUPS
HID = 5120
BLK = 1280
QW = HEADS * HEAD
KVW = GROUPS * HEAD
FFW = 896
FF_TILES = 27
SLOTS = 256
TOK = 1601
ROWS = 2 * TOK * BATCH
STEP = 2 * TOK - 2
WIN = STEP + 16
VMEM_LIMIT = 67043328
PIECE = 640
SCALE = HEAD ** -0.5
N_LOCAL = 11
N_REMOTE = 29


def rope_freqs(head_dim):
    freq_list = []
    for index in range(head_dim // 2):
        base_freq = 1.0 / (ROPE_THETA ** (2.0 * index / head_dim))
        wave_len = 2.0 * math.pi / base_freq
        if wave_len < 2048.0:
            freq_list.append(base_freq)
        elif wave_len > 8192.0:
            freq_list.append(base_freq / 8.0)
        else:
            smooth = (8192.0 / wave_len - 1.0) / 3.0
            freq_list.append((1.0 - smooth) * base_freq / 8.0 + smooth * base_freq)
    return np.array(freq_list + freq_list, dtype=np.float32)


def cos_sin(angle):
    turns = jnp.floor(angle * (2.0 / math.pi) + 0.5)
    r = ((angle - turns * 1.5703125) - turns * 4.837512969970703125e-4) - turns * 7.54978995489188216e-8
    z = r * r
    s = r + r * z * ((-1.9515295891e-4 * z + 8.3321608736e-3) * z - 1.6666654611e-1)
    c = 1.0 - 0.5 * z + z * z * ((2.443315711809948e-5 * z - 1.388731625493765e-3) * z + 4.166664568298827e-2)
    quarter = turns - 4.0 * jnp.floor(turns * 0.25)
    swap = jnp.logical_or(quarter == 1.0, quarter == 3.0)
    cos_t = jnp.where(swap, s, c) * jnp.where(jnp.logical_or(quarter == 1.0, quarter == 2.0), -1.0, 1.0)
    sin_t = jnp.where(swap, c, s) * jnp.where(quarter >= 2.0, -1.0, 1.0)
    return cos_t, sin_t


def dot(a, b):
    return jnp.dot(a, b, preferred_element_type=F32)


def bf(value):
    return value.astype(BF16).astype(F32)


def kernel(x_h, n0_h, n1_h, n2_h, n3_h, qn_h, rope_h, gates_ref, seq_ref, vis_ref,
           ks_h, vs_h, kx_h, vx_h,
           wq1_h, wk_h, wv_h, wo1_h, wg1_h, wu1_h, wd1_h,
           wq2_h, wo2_h, wg2_h, wu2_h, wd2_h,
           h_out, k_out, v_out,
           x_v, kv_v, raw_v, qn_v, gains_v, rope_v, buf_a, buf_o,
           u_v, qbd_v, qc_v, o_v, s_self, p_self, s_cross, p_cross,
           comb, part, rs_buf, hs_buf, y_buf, zr_buf, gather, hbuf,
           lsem, wsem, osem, send_sem, recv_sem):
    tp = lax.axis_index("tp")
    kv = lax.axis_index("kv")
    core = lax.rem(tp, 2)
    side = tp // 2
    mate = {"tp": tp + 1 - 2 * core}
    across = {"tp": lax.rem(tp + 2, 4)}
    around = [lax.rem(kv + j, 4) for j in (3, 2, 1)]
    counts = {"remote": 0, "local": 0}

    def remote(src, dst, device):
        i = counts["remote"]
        counts["remote"] += 1
        copy = pltpu.make_async_remote_copy(src_ref=src, dst_ref=dst, send_sem=send_sem.at[i],
                                            recv_sem=recv_sem.at[i], device_id=device, device_id_type=MESH)
        copy.start()
        return copy

    def local(src, dst):
        i = counts["local"]
        counts["local"] += 1
        copy = pltpu.make_async_copy(src, dst, lsem.at[i])
        copy.start()
        return copy

    def wait_all(copies):
        for copy in copies:
            copy.wait()

    ff_off = pl.multiple_of(jnp.minimum(kv * 7, FF_TILES - 7) * 128, 128)

    def copy_a(w_h, c):
        return pltpu.make_async_copy(w_h.at[pl.ds(c * BLK, BLK), :], buf_a.at[c], wsem.at[c])

    def copies_a(w_h):
        return [copy_a(w_h, c) for c in range(4)]

    def copy_o(w_h, c):
        return pltpu.make_async_copy(w_h.at[:, pl.ds(c * BLK, BLK)], buf_o.at[c], wsem.at[4 + c])

    def copies_o(w_h):
        return [copy_o(w_h, c) for c in range(4)]

    def copies_up(wg_h, wu_h, gu):
        return [pltpu.make_async_copy(w_h.at[pl.ds(c * BLK, BLK), pl.ds(ff_off, FFW)], gu.at[c, :, pl.ds(i * FFW, FFW)],
                                      wsem.at[8 + 2 * c + i]) for c in range(4) for i, w_h in enumerate((wg_h, wu_h))]

    def copies_down(wd_h, dn):
        return [pltpu.make_async_copy(wd_h.at[pl.ds(ff_off, FFW), pl.ds(c * BLK, BLK)], dn.at[c], wsem.at[16 + c])
                for c in range(4)]

    def start_all(copies):
        for copy in copies:
            copy.start()

    first = [local(x_h, x_v), local(n0_h, raw_v.at[0]), local(rope_h, rope_v.at[0])]
    later = [local(n1_h, raw_v.at[1]), local(n2_h, raw_v.at[2]), local(n3_h, raw_v.at[3]), local(qn_h, qn_v)]
    rows = lax.broadcasted_iota(jnp.int32, (BATCH, 1), 0)
    lanes = lax.broadcasted_iota(jnp.int32, (BATCH, HEAD), 1)
    seq = jnp.zeros((BATCH, 1), jnp.int32)
    for b in range(BATCH):
        seq = jnp.where(rows == b, seq_ref[b], seq)
    seen_here = jnp.zeros((BATCH, 1), jnp.int32)
    seen = jnp.zeros((BATCH, 1), jnp.int32)
    for b in range(BATCH):
        seen_here = jnp.where(rows == b, vis_ref[kv, b], seen_here)
        seen = jnp.where(rows == b, vis_ref[0, b] + vis_ref[1, b] + vis_ref[2, b] + vis_ref[3, b], seen)

    def norm_to_u(slot, gain_row):
        total = jnp.zeros((BATCH, 1), F32)
        for p in range(8):
            h = hbuf[slot, p]
            total = total + jnp.sum(h * h, axis=-1, keepdims=True)
        scale = lax.rsqrt(total / HID + NORM_EPS)
        for p in range(8):
            for i in range(5):
                span = slice(i * HEAD, (i + 1) * HEAD)
                row = 5 * p + i
                u_v[p, :, span] = hbuf[slot, p, :, span] * scale * gains_v[gain_row, row:row + 1, :]

    def u_block(c):
        return jnp.concatenate([u_v[2 * c], u_v[2 * c + 1]], axis=-1).astype(BF16)

    def put_queries(query):
        zero = jnp.zeros((BATCH, HEAD), F32)
        for r in range(HEADS):
            g = r // PER
            qbd_v[r * BATCH:(r + 1) * BATCH, g * HEAD:(g + 1) * HEAD] = query[r]
            qbd_v[r * BATCH:(r + 1) * BATCH, (1 - g) * HEAD:(2 - g) * HEAD] = zero

    def scores(keys, s_ref):
        q = qbd_v[...].astype(BF16)
        for b in range(BATCH):
            k_cat = jnp.concatenate([keys[b, 0], keys[b, 1]], axis=-1)
            s = lax.dot_general(q, k_cat, (((1,), (1,)), ((), ())), preferred_element_type=F32)
            for r in range(HEADS):
                s_ref[r, b:b + 1, :] = s[r * BATCH + b:r * BATCH + b + 1, :]

    def weigh(values, p_ref):
        for b in range(BATCH):
            v_cat = jnp.concatenate([values[b, 0], values[b, 1]], axis=-1)
            o = dot(p_ref[...], v_cat)
            for r in range(HEADS):
                g = r // PER
                o_v[r, b:b + 1, :] = o[r * BATCH + b:r * BATCH + b + 1, g * HEAD:(g + 1) * HEAD]

    def put_partials(slot, outs, tops, totals):
        stats = jnp.zeros((BATCH, HEAD), F32)
        for r in range(HEADS):
            comb[slot, kv, :, r * HEAD:(r + 1) * HEAD] = outs[r]
            stats = jnp.where(lanes == r, tops[r], stats)
            stats = jnp.where(lanes == HEAD // 2 + r, totals[r], stats)
        comb[slot, kv, :, QW:QW + HEAD] = stats

    def exchange_partials(slot):
        counts["remote"] = 0
        with jax.named_scope("comb_exchange"):
            wait_all([remote(comb.at[slot, kv], comb.at[slot, kv], {"kv": peer}) for peer in around])
        best = comb[slot, 0, :, QW:QW + HEAD]
        for s in range(1, 4):
            best = jnp.maximum(best, comb[slot, s, :, QW:QW + HEAD])
        best = jnp.where(lanes < HEAD // 2, best, 0.0)
        weight = [jnp.exp(jnp.where(lanes < HEAD // 2, comb[slot, s, :, QW:QW + HEAD] - best, 0.0)) for s in range(4)]
        norm = sum(pltpu.roll(comb[slot, s, :, QW:QW + HEAD], HEAD // 2, 1) * weight[s] for s in range(4))
        inverse = 1.0 / jnp.where(norm > 0, norm, 1.0)
        heads = []
        for r in range(HEADS):
            mixed = sum(comb[slot, s, :, r * HEAD:(r + 1) * HEAD] * weight[s][:, r:r + 1] for s in range(4))
            heads.append(mixed * inverse[:, r:r + 1])
        return jnp.concatenate(heads, axis=-1).astype(BF16)

    def half_sums(slot, left, w_ref, ready):
        def run(c):
            out = dot(left, w_ref[c])
            part[slot, 2 * c] = out[:, :PIECE]
            part[slot, 2 * c + 1] = out[:, PIECE:]
        copies = []
        with jax.named_scope("halves"):
            for i in range(2):
                run(2 * (1 - core) + i)
                copies.append(remote(part.at[slot, pl.ds(4 * (1 - core) + 2 * i, 2)], rs_buf.at[slot, pl.ds(2 * i, 2)], mate))
            for i in range(2):
                run(2 * core + i)
                copies[i].wait()
                for j in (2 * i, 2 * i + 1):
                    hs_buf[slot, j] = part[slot, 4 * core + j] + rs_buf[slot, j]
                ready(i)

    def reduce_plane(slot, left, w_ref, h_from, h_to, finish):
        sends = []
        half_sums(slot, left, w_ref, lambda i: sends.append(
            remote(hs_buf.at[slot, pl.ds(2 * i, 2)], y_buf.at[slot // 2, pl.ds(2 * i, 2)], across)))
        with jax.named_scope("reduce_plane"):
            backs = []
            for i in range(2):
                sends[i].wait()
                for j in (2 * i, 2 * i + 1):
                    p = 4 * core + j
                    hbuf[h_to, p] = bf(finish(hbuf[h_from, p], hs_buf[slot, j] + y_buf[slot // 2, j]))
                span = hbuf.at[h_to, pl.ds(4 * core + 2 * i, 2)]
                backs.append(remote(span, span, mate))
            wait_all(backs)

    def scatter_all(slot):
        with jax.named_scope("all_z"):
            i_z = slot // 2
            copies = [remote(hs_buf.at[slot, peer], zr_buf.at[i_z, kv], {"kv": peer}) for peer in around]
            zr_buf[i_z, kv] = hs_buf[slot, kv]
            wait_all(copies)
            gather[i_z, side, 4 * core + kv] = zr_buf[i_z, 0] + zr_buf[i_z, 1] + zr_buf[i_z, 2] + zr_buf[i_z, 3]

    def gather_all(slot, h_from, h_to, finish):
        i_z = slot // 2
        with jax.named_scope("all_gather"):
            own = gather.at[i_z, side, 4 * core + kv]
            relays = [remote(own, own, mate)]
            sends = []
            for j in (2, 1, 3):
                to = lax.rem(kv + j, 4)
                sends.append((remote(own, own, {"kv": to}), side, j))
            for j in (2, 1, 3):
                to = lax.rem(kv + j, 4)
                sends.append((remote(own, own, {"kv": to, "tp": lax.rem(tp + 2, 4)}), 1 - side, j))
            sends.insert(0, (remote(own, own, across), 1 - side, 0))
            order = sorted(range(7), key=lambda n: (sends[n][2] == 2, n))
            for n in order:
                copy, s, j = sends[n]
                copy.wait()
                got = gather.at[i_z, s, 4 * core + lax.rem(kv + 4 - j, 4)]
                relays.append(remote(got, got, mate))
            wait_all(relays)
        for p in range(8):
            hbuf[h_to, p] = bf(finish(hbuf[h_from, p], gather[i_z, 0, p] + gather[i_z, 1, p]))

    def mlp(slot, gain_row, h_slot, gu, dn, up, down):
        norm_to_u(h_slot, gain_row)
        acc = jnp.zeros((BATCH, 2 * FFW), F32)
        with jax.named_scope("gate_up"):
            wait_all(up)
            for c in range(4):
                acc = acc + dot(u_block(c), gu[c])
        gate, upper = acc[:, :FFW], acc[:, FFW:]
        act = gate * (1.0 / (1.0 + jnp.exp(-gate))) * upper
        keep = jnp.logical_or(kv < 3, lax.broadcasted_iota(jnp.int32, (BATCH, FFW), 1) >= 128)
        act = jnp.where(keep, act, 0.0).astype(BF16)
        wait_all(down)
        half_sums(slot, act, dn, lambda i: None)
        scatter_all(slot)

    def new_copies():
        return [pltpu.make_async_copy(kv_v.at[i], out, osem.at[i]) for i, out in enumerate((k_out, v_out))]

    def self_attention(wkv, ks, vs, gu):
        def copies_q(c):
            return [copy_a(wq1_h, c)] + [
                pltpu.make_async_copy(w_h.at[pl.ds(c * BLK, BLK), :], wkv.at[c, :, pl.ds(i * KVW, KVW)], wsem.at[20 + 2 * c + i])
                for i, w_h in enumerate((wk_h, wv_h))]

        for c in range(4):
            start_all(copies_q(c))

        barrier = pltpu.get_barrier_semaphore()
        peers = [{"kv": peer} for peer in around] + [{"kv": peer, "tp": lax.rem(tp + 2, 4)} for peer in around] + [mate, across]
        for peer in peers:
            pl.semaphore_signal(barrier, inc=1, device_id=peer, device_id_type=MESH)

        with jax.named_scope("first_wait"):
            wait_all(first)
        for p in range(8):
            hbuf[0, p] = x_v[:, p * PIECE:(p + 1) * PIECE].astype(F32)
        gains_v[0] = raw_v[0].astype(F32)
        norm_to_u(0, 0)
        angles = seq.astype(F32) * rope_v[0]
        cos_t, sin_t = cos_sin(angles)
        rope_v[1] = cos_t
        rope_v[2] = sin_t * jnp.where(lanes < HEAD // 2, -1.0, 1.0)
        wait_all(later)
        for i in range(1, 4):
            gains_v[i] = raw_v[i].astype(F32)

        def rope(z):
            return bf(z * rope_v[1] + pltpu.roll(z, HEAD // 2, 1) * rope_v[2])

        acc_q = jnp.zeros((BATCH, QW), F32)
        acc_kv = jnp.zeros((BATCH, 2 * KVW), F32)
        with jax.named_scope("qkv"):
            for c in range(4):
                wait_all(copies_q(c))
                if c == 1:
                    caches = [local(ks_h, ks), local(vs_h, vs)]
                elif c == 2:
                    start_all([copy_o(wo1_h, i) for i in range(4)])
                left = u_block(c)
                acc_q = acc_q + dot(left, buf_a[c])
                acc_kv = acc_kv + dot(left, wkv[c])
        query = [rope(acc_q[:, r * HEAD:(r + 1) * HEAD]) for r in range(HEADS)]
        key_new = [rope(acc_kv[:, g * HEAD:(g + 1) * HEAD]) for g in range(GROUPS)]
        val_new = [bf(acc_kv[:, KVW + g * HEAD:KVW + (g + 1) * HEAD]) for g in range(GROUPS)]
        for g in range(GROUPS):
            kv_v[0, :, g * HEAD:(g + 1) * HEAD] = key_new[g].astype(BF16)
            kv_v[1, :, g * HEAD:(g + 1) * HEAD] = val_new[g].astype(BF16)
        put_queries(query)
        wait_all(caches)
        with jax.named_scope("self_scores"):
            scores(ks, s_self)
        slot_ids = kv * SLOTS + lax.broadcasted_iota(jnp.int32, (BATCH, SLOTS), 1)
        visible = slot_ids < seq
        owner = jnp.logical_and(seq >= kv * SLOTS, seq < (kv + 1) * SLOTS)
        tops, totals, news = [], [], []
        for pair in range(HEADS // 2):
            both = []
            for r in (2 * pair, 2 * pair + 1):
                s = jnp.where(visible, s_self[r] * SCALE, MASK_VALUE)
                new = jnp.sum(query[r] * key_new[r // PER], axis=-1, keepdims=True) * SCALE
                new = jnp.where(owner, new, MASK_VALUE)
                top = jnp.maximum(jnp.max(s, axis=-1, keepdims=True), new)
                prob = jnp.where(visible, jnp.exp(s - top), 0.0)
                new_prob = jnp.where(owner, jnp.exp(new - top), 0.0)
                tops.append(top)
                totals.append(jnp.sum(prob, axis=-1, keepdims=True) + new_prob)
                news.append(new_prob)
                both.append(prob)
            p_self[2 * pair * BATCH:(2 * pair + 2) * BATCH, :] = jnp.concatenate(both, axis=0).astype(BF16)
        with jax.named_scope("self_weigh"):
            weigh(vs, p_self)
        outs = [o_v[r] + news[r] * val_new[r // PER] for r in range(HEADS)]
        with jax.named_scope("barrier"):
            pl.semaphore_wait(barrier, len(peers))
        put_partials(0, outs, tops, totals)

    def self_rest(dn, gu):
        start_all(new_copies())
        start_all(copies_up(wg1_h, wu1_h, gu))
        start_all(copies_down(wd1_h, dn))
        start_all(copies_a(wq2_h))
        attn = exchange_partials(0)
        wait_all(copies_o(wo1_h))
        reduce_plane(0, attn, buf_o, 0, 1, lambda h, s: h + s)
        start_all(copies_o(wo2_h))
        mlp(1, 1, 1, gu, dn, copies_up(wg1_h, wu1_h, gu), copies_down(wd1_h, dn))

    up_space = pltpu.VMEM((4, BLK, 2 * FFW), BF16)
    down_space = pltpu.VMEM((4, FFW, BLK), BF16)

    def phase_one(gu):
        pl.run_scoped(functools.partial(self_attention, gu=gu), pltpu.VMEM((4, BLK, 2 * KVW), BF16),
                      pltpu.VMEM((BATCH, GROUPS, SLOTS, HEAD), BF16), pltpu.VMEM((BATCH, GROUPS, SLOTS, HEAD), BF16))
        pl.run_scoped(functools.partial(self_rest, gu=gu), down_space)

    pl.run_scoped(phase_one, up_space)

    visible_tile = seen_here > 0
    row_on = jnp.where(seen > 0, 1.0, 0.0)

    def scope_two(kx, vx):
        caches = [local(kx_h, kx), local(vx_h, vx)]
        gather_all(1, 1, 2, lambda h, s: h + s)
        norm_to_u(2, 2)
        acc = jnp.zeros((BATCH, QW), F32)
        with jax.named_scope("q_cross"):
            wait_all(copies_a(wq2_h))
            for c in range(4):
                acc = acc + dot(u_block(c), buf_a[c])
        query = []
        for r in range(HEADS):
            z = acc[:, r * HEAD:(r + 1) * HEAD]
            z = z * lax.rsqrt(jnp.mean(z * z, axis=-1, keepdims=True) + NORM_EPS) * qn_v[...].astype(F32)
            query.append(bf(z))
        for r in range(HEADS):
            qc_v[r * BATCH:(r + 1) * BATCH, :] = query[r]
        with jax.named_scope("cross_scores"):
            wait_all(caches)
            q = qc_v[...].astype(BF16)
            for b in range(BATCH):
                s = lax.dot_general(q, kx[b * STEP:b * STEP + WIN, :], (((1,), (1,)), ((), ())),
                                    preferred_element_type=F32)
                for r in range(HEADS):
                    s_cross[r, b:b + 1, :] = s[r * BATCH + b:r * BATCH + b + 1, :]
        place = lax.broadcasted_iota(jnp.int32, (BATCH, WIN), 1) - 2 * lax.broadcasted_iota(jnp.int32, (BATCH, WIN), 0)
        inside = jnp.logical_and(place >= 0, place < 2 * TOK)
        tops, totals = [], []
        for pair in range(HEADS // 2):
            both = []
            for r in (2 * pair, 2 * pair + 1):
                mine = jnp.logical_and(inside, lax.rem(place + 16, 2) == r // PER)
                s = jnp.where(mine, s_cross[r] * SCALE, MASK_VALUE)
                top = jnp.max(s, axis=-1, keepdims=True)
                prob = jnp.where(mine, jnp.exp(s - top), 0.0)
                tops.append(jnp.where(visible_tile, top, MASK_VALUE))
                totals.append(jnp.where(visible_tile, jnp.sum(prob, axis=-1, keepdims=True), 0.0))
                both.append(prob)
            p_cross[2 * pair * BATCH:(2 * pair + 2) * BATCH, :] = jnp.concatenate(both, axis=0).astype(BF16)
        with jax.named_scope("cross_weigh"):
            for b in range(BATCH):
                o = dot(p_cross[...], vx[b * STEP:b * STEP + WIN, :])
                for r in range(HEADS):
                    o_v[r, b:b + 1, :] = o[r * BATCH + b:r * BATCH + b + 1, :]
        outs = [jnp.where(visible_tile, o_v[r], 0.0) for r in range(HEADS)]
        put_partials(1, outs, tops, totals)

    pl.run_scoped(scope_two, pltpu.VMEM((ROWS, HEAD), BF16), pltpu.VMEM((ROWS, HEAD), BF16))

    def gate(i):
        return jnp.tanh(jnp.full((BATCH, HEAD), gates_ref[i], F32))[:, 0:1] * row_on

    def scope_three(gu, dn):
        start_all(copies_up(wg2_h, wu2_h, gu))
        start_all(copies_down(wd2_h, dn))
        attn = exchange_partials(1)
        wait_all(copies_o(wo2_h))
        reduce_plane(2, attn, buf_o, 2, 3, lambda h, s: h + gate(0) * s)
        mlp(3, 3, 3, gu, dn, copies_up(wg2_h, wu2_h, gu), copies_down(wd2_h, dn))

    pl.run_scoped(scope_three, up_space, down_space)
    gather_all(3, 3, 4, lambda h, s: h + gate(1) * s)
    with jax.named_scope("put_h"):
        for p in range(8):
            x_v[:, p * PIECE:(p + 1) * PIECE] = hbuf[4, p].astype(BF16)
        put = pltpu.make_async_copy(x_v, h_out, osem.at[2])
        put.start()
        put.wait()
        for copy in new_copies():
            copy.wait()


def put_out(h_in, k_in, v_in, h_out, k_out, v_out):
    h_out[...] = h_in[...]
    for src, dst in ((k_in, k_out), (v_in, v_out)):
        dst[...] = src[...].astype(F32).reshape(BATCH, GROUPS, HEAD).astype(BF16)


def solution(mesh):
    rows_spec = P('dp', None)
    cache_spec = P('dp', 'tp', 'kv', None)
    new_spec = P('dp', 'tp', None)
    col_spec = P(None, 'tp')
    row_spec = P('tp', None)
    vec_spec = P(None)
    in_specs = (rows_spec, cache_spec, cache_spec, P('dp'), cache_spec, cache_spec, rows_spec,
                vec_spec, col_spec, col_spec, col_spec, row_spec, vec_spec, col_spec, col_spec, row_spec,
                vec_spec, col_spec, vec_spec, row_spec, vec_spec, vec_spec, col_spec, col_spec, row_spec)
    out_specs = (rows_spec, new_spec, new_spec)

    def device_step(x, ks_cache, vs_cache, seq_len, kx_cache, vx_cache, tile_vis, attn_norm, wq_self, wk_self, wv_self, wo_self, mlp_norm, wg_self, wu_self, wd_self, xattn_norm, wq_cross, q_norm, wo_cross, cross_gates, xmlp_norm, wg_cross, wu_cross, wd_cross):
        freqs = jnp.asarray(np.tile(rope_freqs(HEAD)[None, :], (BATCH, 1)))
        norms = [gain.reshape(HID // HEAD, HEAD) for gain in (attn_norm, mlp_norm, xattn_norm, xmlp_norm)]
        kx_rows, vx_rows = [cache.transpose(0, 2, 1, 3).reshape(ROWS, HEAD) for cache in (kx_cache, vx_cache)]
        hbm = pl.BlockSpec(memory_space=pl.ANY)
        smem = pl.BlockSpec(memory_space=pltpu.SMEM)
        vmem = pl.BlockSpec(memory_space=pltpu.VMEM)
        piece = (8, BATCH, PIECE)
        scratch = [
            pltpu.VMEM((BATCH, HID), BF16), pltpu.VMEM((2, BATCH, KVW), BF16), pltpu.VMEM((4, HID // HEAD, HEAD), BF16), pltpu.VMEM((1, HEAD), BF16),
            pltpu.VMEM((4, HID // HEAD, HEAD), F32), pltpu.VMEM((3, BATCH, HEAD), F32),
            pltpu.VMEM((4, BLK, BLK), BF16), pltpu.VMEM((4, BLK, BLK), BF16),
            pltpu.VMEM(piece, F32), pltpu.VMEM((HEADS * BATCH, 2 * HEAD), F32), pltpu.VMEM((HEADS * BATCH, HEAD), F32), pltpu.VMEM((HEADS, BATCH, HEAD), F32),
            pltpu.VMEM((HEADS, BATCH, SLOTS), F32), pltpu.VMEM((HEADS * BATCH, SLOTS), BF16),
            pltpu.VMEM((HEADS, BATCH, WIN), F32), pltpu.VMEM((HEADS * BATCH, WIN), BF16),
            pltpu.VMEM((2, 4, BATCH, QW + HEAD), F32),
            pltpu.VMEM((4,) + piece, F32), pltpu.VMEM((4, 4, BATCH, PIECE), F32),
            pltpu.VMEM((4, 4, BATCH, PIECE), F32), pltpu.VMEM((2, 4, BATCH, PIECE), F32),
            pltpu.VMEM((2, 4, BATCH, PIECE), F32), pltpu.VMEM((2, 2) + piece, F32),
            pltpu.VMEM((5,) + piece, F32),
            pltpu.SemaphoreType.DMA((N_LOCAL,)), pltpu.SemaphoreType.DMA((28,)), pltpu.SemaphoreType.DMA((3,)), pltpu.SemaphoreType.DMA((N_REMOTE,)), pltpu.SemaphoreType.DMA((N_REMOTE,)),
        ]
        h, key_new, val_new = pl.pallas_call(
            kernel,
            out_shape=(jax.ShapeDtypeStruct((BATCH, HID), BF16), jax.ShapeDtypeStruct((BATCH, KVW), BF16),
                       jax.ShapeDtypeStruct((BATCH, KVW), BF16)),
            in_specs=[hbm] * 7 + [smem] * 3 + [hbm] * 16,
            out_specs=(hbm, hbm, hbm),
            scratch_shapes=scratch,
            compiler_params=pltpu.CompilerParams(collective_id=0, has_side_effects=True, vmem_limit_bytes=VMEM_LIMIT),
        )(x, *norms, q_norm.reshape(1, HEAD), freqs, cross_gates, seq_len, tile_vis.T, ks_cache, vs_cache, kx_rows, vx_rows,
          wq_self, wk_self, wv_self, wo_self, wg_self, wu_self, wd_self, wq_cross, wo_cross, wg_cross, wu_cross, wd_cross)
        return pl.pallas_call(
            put_out,
            out_shape=(jax.ShapeDtypeStruct((BATCH, HID), BF16), jax.ShapeDtypeStruct((BATCH, GROUPS, HEAD), BF16),
                       jax.ShapeDtypeStruct((BATCH, GROUPS, HEAD), BF16)),
            in_specs=[vmem] * 3, out_specs=(vmem,) * 3)(h, key_new, val_new)

    return jax.shard_map(device_step, mesh=mesh, in_specs=in_specs, out_specs=out_specs, check_vma=False)
```

```python
import functools
import math
import numpy as np
import jax
import jax.numpy as jnp
from jax import lax
from jax.experimental import pallas as pl
from jax.experimental.pallas import tpu as pltpu
from jax.sharding import PartitionSpec as P

NORM_EPS = 1e-5
ROPE_THETA = 500000.0
MASK_VALUE = -1e30
MESH = pl.DeviceIdType.MESH
BF16 = jnp.bfloat16
F32 = jnp.float32

BATCH = 8
HEAD = 128
HEADS = 10
GROUPS = 2
PER = HEADS // GROUPS
HID = 5120
BLK = 1280
QW = HEADS * HEAD
KVW = GROUPS * HEAD
FFW = 896
FF_TILES = 27
SLOTS = 256
TOK = 1601
ROWS = 2 * TOK * BATCH
STEP = 2 * TOK - 2
WIN = STEP + 16
VMEM_LIMIT = 67043328
PIECE = 640
SCALE = HEAD ** -0.5
N_LOCAL = 11
N_REMOTE = 29


def rope_freqs(head_dim):
    freq_list = []
    for index in range(head_dim // 2):
        base_freq = 1.0 / (ROPE_THETA ** (2.0 * index / head_dim))
        wave_len = 2.0 * math.pi / base_freq
        if wave_len < 2048.0:
            freq_list.append(base_freq)
        elif wave_len > 8192.0:
            freq_list.append(base_freq / 8.0)
        else:
            smooth = (8192.0 / wave_len - 1.0) / 3.0
            freq_list.append((1.0 - smooth) * base_freq / 8.0 + smooth * base_freq)
    return np.array(freq_list + freq_list, dtype=np.float32)


def cos_sin(angle):
    turns = jnp.floor(angle * (2.0 / math.pi) + 0.5)
    r = ((angle - turns * 1.5703125) - turns * 4.837512969970703125e-4) - turns * 7.54978995489188216e-8
    z = r * r
    s = r + r * z * ((-1.9515295891e-4 * z + 8.3321608736e-3) * z - 1.6666654611e-1)
    c = 1.0 - 0.5 * z + z * z * ((2.443315711809948e-5 * z - 1.388731625493765e-3) * z + 4.166664568298827e-2)
    quarter = turns - 4.0 * jnp.floor(turns * 0.25)
    swap = jnp.logical_or(quarter == 1.0, quarter == 3.0)
    cos_t = jnp.where(swap, s, c) * jnp.where(jnp.logical_or(quarter == 1.0, quarter == 2.0), -1.0, 1.0)
    sin_t = jnp.where(swap, c, s) * jnp.where(quarter >= 2.0, -1.0, 1.0)
    return cos_t, sin_t


def dot(a, b):
    return jnp.dot(a, b, preferred_element_type=F32)


def bf(value):
    return value.astype(BF16).astype(F32)


def kernel(x_h, n0_h, n1_h, n2_h, n3_h, qn_h, rope_h, gates_ref, seq_ref, vis_ref,
           ks_h, vs_h, kx_h, vx_h,
           wq1_h, wk_h, wv_h, wo1_h, wg1_h, wu1_h, wd1_h,
           wq2_h, wo2_h, wg2_h, wu2_h, wd2_h,
           h_out, k_out, v_out,
           x_v, kv_v, raw_v, qn_v, gains_v, rope_v, buf_a, buf_o,
           u_v, qbd_v, qc_v, o_v, s_self, p_self, s_cross, p_cross,
           comb, part, rs_buf, hs_buf, y_buf, zr_buf, gather, hbuf,
           lsem, wsem, osem, send_sem, recv_sem):
    tp = lax.axis_index("tp")
    kv = lax.axis_index("kv")
    core = lax.rem(tp, 2)
    side = tp // 2
    mate = {"tp": tp + 1 - 2 * core}
    across = {"tp": lax.rem(tp + 2, 4)}
    around = [lax.rem(kv + j, 4) for j in (3, 2, 1)]
    counts = {"remote": 0, "local": 0}

    def remote(src, dst, device):
        i = counts["remote"]
        counts["remote"] += 1
        copy = pltpu.make_async_remote_copy(src_ref=src, dst_ref=dst, send_sem=send_sem.at[i],
                                            recv_sem=recv_sem.at[i], device_id=device, device_id_type=MESH)
        copy.start()
        return copy

    def local(src, dst):
        i = counts["local"]
        counts["local"] += 1
        copy = pltpu.make_async_copy(src, dst, lsem.at[i])
        copy.start()
        return copy

    def wait_all(copies):
        for copy in copies:
            copy.wait()

    ff_off = pl.multiple_of(jnp.minimum(kv * 7, FF_TILES - 7) * 128, 128)

    def copy_a(w_h, c):
        return pltpu.make_async_copy(w_h.at[pl.ds(c * BLK, BLK), :], buf_a.at[c], wsem.at[c])

    def copies_a(w_h):
        return [copy_a(w_h, c) for c in range(4)]

    def copy_o(w_h, c):
        return pltpu.make_async_copy(w_h.at[:, pl.ds(c * BLK, BLK)], buf_o.at[c], wsem.at[4 + c])

    def copies_o(w_h):
        return [copy_o(w_h, c) for c in range(4)]

    def copies_up(wg_h, wu_h, gu):
        return [pltpu.make_async_copy(w_h.at[pl.ds(c * BLK, BLK), pl.ds(ff_off, FFW)], gu.at[c, :, pl.ds(i * FFW, FFW)],
                                      wsem.at[8 + 2 * c + i]) for c in range(4) for i, w_h in enumerate((wg_h, wu_h))]

    def copies_down(wd_h, dn):
        return [pltpu.make_async_copy(wd_h.at[pl.ds(ff_off, FFW), pl.ds(c * BLK, BLK)], dn.at[c], wsem.at[16 + c])
                for c in range(4)]

    def start_all(copies):
        for copy in copies:
            copy.start()

    first = [local(x_h, x_v), local(n0_h, raw_v.at[0]), local(rope_h, rope_v.at[0])]
    later = [local(n1_h, raw_v.at[1]), local(n2_h, raw_v.at[2]), local(n3_h, raw_v.at[3]), local(qn_h, qn_v)]
    rows = lax.broadcasted_iota(jnp.int32, (BATCH, 1), 0)
    lanes = lax.broadcasted_iota(jnp.int32, (BATCH, HEAD), 1)
    seq = jnp.zeros((BATCH, 1), jnp.int32)
    for b in range(BATCH):
        seq = jnp.where(rows == b, seq_ref[b], seq)
    seen_here = jnp.zeros((BATCH, 1), jnp.int32)
    seen = jnp.zeros((BATCH, 1), jnp.int32)
    for b in range(BATCH):
        seen_here = jnp.where(rows == b, vis_ref[kv, b], seen_here)
        seen = jnp.where(rows == b, vis_ref[0, b] + vis_ref[1, b] + vis_ref[2, b] + vis_ref[3, b], seen)

    def norm_to_u(slot, gain_row):
        total = jnp.zeros((BATCH, 1), F32)
        for p in range(8):
            h = hbuf[slot, p]
            total = total + jnp.sum(h * h, axis=-1, keepdims=True)
        scale = lax.rsqrt(total / HID + NORM_EPS)
        for p in range(8):
            for i in range(5):
                span = slice(i * HEAD, (i + 1) * HEAD)
                row = 5 * p + i
                u_v[p, :, span] = hbuf[slot, p, :, span] * scale * gains_v[gain_row, row:row + 1, :]

    def u_block(c):
        return jnp.concatenate([u_v[2 * c], u_v[2 * c + 1]], axis=-1).astype(BF16)

    def put_queries(query):
        zero = jnp.zeros((BATCH, HEAD), F32)
        for r in range(HEADS):
            g = r // PER
            qbd_v[r * BATCH:(r + 1) * BATCH, g * HEAD:(g + 1) * HEAD] = query[r]
            qbd_v[r * BATCH:(r + 1) * BATCH, (1 - g) * HEAD:(2 - g) * HEAD] = zero

    def scores(keys, s_ref):
        q = qbd_v[...].astype(BF16)
        for b in range(BATCH):
            k_cat = jnp.concatenate([keys[b, 0], keys[b, 1]], axis=-1)
            s = lax.dot_general(q, k_cat, (((1,), (1,)), ((), ())), preferred_element_type=F32)
            for r in range(HEADS):
                s_ref[r, b:b + 1, :] = s[r * BATCH + b:r * BATCH + b + 1, :]

    def weigh(values, p_ref):
        for b in range(BATCH):
            v_cat = jnp.concatenate([values[b, 0], values[b, 1]], axis=-1)
            o = dot(p_ref[...], v_cat)
            for r in range(HEADS):
                g = r // PER
                o_v[r, b:b + 1, :] = o[r * BATCH + b:r * BATCH + b + 1, g * HEAD:(g + 1) * HEAD]

    def put_partials(slot, outs, tops, totals):
        stats = jnp.zeros((BATCH, HEAD), F32)
        for r in range(HEADS):
            comb[slot, kv, :, r * HEAD:(r + 1) * HEAD] = outs[r]
            stats = jnp.where(lanes == r, tops[r], stats)
            stats = jnp.where(lanes == HEAD // 2 + r, totals[r], stats)
        comb[slot, kv, :, QW:QW + HEAD] = stats

    def exchange_partials(slot):
        counts["remote"] = 0
        with jax.named_scope("comb_exchange"):
            wait_all([remote(comb.at[slot, kv], comb.at[slot, kv], {"kv": peer}) for peer in around])
        best = comb[slot, 0, :, QW:QW + HEAD]
        for s in range(1, 4):
            best = jnp.maximum(best, comb[slot, s, :, QW:QW + HEAD])
        best = jnp.where(lanes < HEAD // 2, best, 0.0)
        weight = [jnp.exp(jnp.where(lanes < HEAD // 2, comb[slot, s, :, QW:QW + HEAD] - best, 0.0)) for s in range(4)]
        norm = sum(pltpu.roll(comb[slot, s, :, QW:QW + HEAD], HEAD // 2, 1) * weight[s] for s in range(4))
        inverse = 1.0 / jnp.where(norm > 0, norm, 1.0)
        heads = []
        for r in range(HEADS):
            mixed = sum(comb[slot, s, :, r * HEAD:(r + 1) * HEAD] * weight[s][:, r:r + 1] for s in range(4))
            heads.append(mixed * inverse[:, r:r + 1])
        return jnp.concatenate(heads, axis=-1).astype(BF16)

    def half_sums(slot, left, w_ref, ready):
        def run(c):
            out = dot(left, w_ref[c])
            part[slot, 2 * c] = out[:, :PIECE]
            part[slot, 2 * c + 1] = out[:, PIECE:]
        copies = []
        with jax.named_scope("halves"):
            for i in range(2):
                run(2 * (1 - core) + i)
                copies.append(remote(part.at[slot, pl.ds(4 * (1 - core) + 2 * i, 2)], rs_buf.at[slot, pl.ds(2 * i, 2)], mate))
            for i in range(2):
                run(2 * core + i)
                copies[i].wait()
                for j in (2 * i, 2 * i + 1):
                    hs_buf[slot, j] = part[slot, 4 * core + j] + rs_buf[slot, j]
                ready(i)

    def reduce_plane(slot, left, w_ref, h_from, h_to, finish):
        sends = []
        half_sums(slot, left, w_ref, lambda i: sends.append(
            remote(hs_buf.at[slot, pl.ds(2 * i, 2)], y_buf.at[slot // 2, pl.ds(2 * i, 2)], across)))
        with jax.named_scope("reduce_plane"):
            backs = []
            for i in range(2):
                sends[i].wait()
                for j in (2 * i, 2 * i + 1):
                    p = 4 * core + j
                    hbuf[h_to, p] = bf(finish(hbuf[h_from, p], hs_buf[slot, j] + y_buf[slot // 2, j]))
                span = hbuf.at[h_to, pl.ds(4 * core + 2 * i, 2)]
                backs.append(remote(span, span, mate))
            wait_all(backs)

    def scatter_all(slot):
        with jax.named_scope("all_z"):
            i_z = slot // 2
            copies = [remote(hs_buf.at[slot, peer], zr_buf.at[i_z, kv], {"kv": peer}) for peer in around]
            zr_buf[i_z, kv] = hs_buf[slot, kv]
            wait_all(copies)
            gather[i_z, side, 4 * core + kv] = zr_buf[i_z, 0] + zr_buf[i_z, 1] + zr_buf[i_z, 2] + zr_buf[i_z, 3]

    def gather_all(slot, h_from, h_to, finish):
        i_z = slot // 2
        with jax.named_scope("all_gather"):
            own = gather.at[i_z, side, 4 * core + kv]
            relays = [remote(own, own, mate)]
            sends = []
            for j in (2, 1, 3):
                to = lax.rem(kv + j, 4)
                sends.append((remote(own, own, {"kv": to}), side, j))
            for j in (2, 1, 3):
                to = lax.rem(kv + j, 4)
                sends.append((remote(own, own, {"kv": to, "tp": lax.rem(tp + 2, 4)}), 1 - side, j))
            sends.insert(0, (remote(own, own, across), 1 - side, 0))
            order = sorted(range(7), key=lambda n: (sends[n][2] == 2, n))
            for n in order:
                copy, s, j = sends[n]
                copy.wait()
                got = gather.at[i_z, s, 4 * core + lax.rem(kv + 4 - j, 4)]
                relays.append(remote(got, got, mate))
            wait_all(relays)
        for p in range(8):
            hbuf[h_to, p] = bf(finish(hbuf[h_from, p], gather[i_z, 0, p] + gather[i_z, 1, p]))

    def mlp(slot, gain_row, h_slot, gu, dn, up, down):
        norm_to_u(h_slot, gain_row)
        acc = jnp.zeros((BATCH, 2 * FFW), F32)
        with jax.named_scope("gate_up"):
            wait_all(up)
            for c in range(4):
                acc = acc + dot(u_block(c), gu[c])
        gate, upper = acc[:, :FFW], acc[:, FFW:]
        act = gate * (1.0 / (1.0 + jnp.exp(-gate))) * upper
        keep = jnp.logical_or(kv < 3, lax.broadcasted_iota(jnp.int32, (BATCH, FFW), 1) >= 128)
        act = jnp.where(keep, act, 0.0).astype(BF16)
        wait_all(down)
        half_sums(slot, act, dn, lambda i: None)
        scatter_all(slot)

    def new_copies():
        return [pltpu.make_async_copy(kv_v.at[i], out, osem.at[i]) for i, out in enumerate((k_out, v_out))]

    def self_attention(wkv, ks, vs, gu):
        def copies_q(i):
            src, c, lo = pl.ds(i * PIECE, PIECE), i // 2, (i % 2) * PIECE
            return [pltpu.make_async_copy(wq1_h.at[src, :], buf_a.at[c, pl.ds(lo, PIECE), :], wsem.at[8 + i]),
                    pltpu.make_async_copy(wk_h.at[src, :], wkv.at[c, pl.ds(lo, PIECE), pl.ds(0, KVW)], wsem.at[16 + i]),
                    pltpu.make_async_copy(wv_h.at[src, :], wkv.at[c, pl.ds(lo, PIECE), pl.ds(KVW, KVW)],
                                          wsem.at[i if i < 4 else 20 + i])]

        for i in range(3):
            start_all(copies_q(i))

        barrier = pltpu.get_barrier_semaphore()
        peers = [{"kv": peer} for peer in around] + [{"kv": peer, "tp": lax.rem(tp + 2, 4)} for peer in around] + [mate, across]
        for peer in peers:
            pl.semaphore_signal(barrier, inc=1, device_id=peer, device_id_type=MESH)

        with jax.named_scope("first_wait"):
            wait_all(first)
        for p in range(8):
            hbuf[0, p] = x_v[:, p * PIECE:(p + 1) * PIECE].astype(F32)
        gains_v[0] = raw_v[0].astype(F32)
        norm_to_u(0, 0)
        angles = seq.astype(F32) * rope_v[0]
        cos_t, sin_t = cos_sin(angles)
        rope_v[1] = cos_t
        rope_v[2] = sin_t * jnp.where(lanes < HEAD // 2, -1.0, 1.0)
        wait_all(later)
        for i in range(1, 4):
            gains_v[i] = raw_v[i].astype(F32)

        def rope(z):
            return bf(z * rope_v[1] + pltpu.roll(z, HEAD // 2, 1) * rope_v[2])

        acc_q = jnp.zeros((BATCH, QW), F32)
        acc_kv = jnp.zeros((BATCH, 2 * KVW), F32)
        with jax.named_scope("qkv"):
            for i in range(8):
                wait_all(copies_q(i))
                if i < 5:
                    start_all(copies_q(i + 3))
                elif i == 5:
                    caches = [local(ks_h, ks), local(vs_h, vs)]
                    start_all([copy_o(wo1_h, n) for n in (0, 1)])
                elif i == 6:
                    start_all([copy_o(wo1_h, n) for n in (2, 3)])
                left = u_v[i].astype(BF16)
                c, span = i // 2, slice((i % 2) * PIECE, (i % 2) * PIECE + PIECE)
                acc_q = acc_q + dot(left, buf_a[c, span, :])
                acc_kv = acc_kv + dot(left, wkv[c, span, :])
        query = [rope(acc_q[:, r * HEAD:(r + 1) * HEAD]) for r in range(HEADS)]
        key_new = [rope(acc_kv[:, g * HEAD:(g + 1) * HEAD]) for g in range(GROUPS)]
        val_new = [bf(acc_kv[:, KVW + g * HEAD:KVW + (g + 1) * HEAD]) for g in range(GROUPS)]
        for g in range(GROUPS):
            kv_v[0, :, g * HEAD:(g + 1) * HEAD] = key_new[g].astype(BF16)
            kv_v[1, :, g * HEAD:(g + 1) * HEAD] = val_new[g].astype(BF16)
        put_queries(query)
        wait_all(caches)
        with jax.named_scope("self_scores"):
            scores(ks, s_self)
        slot_ids = kv * SLOTS + lax.broadcasted_iota(jnp.int32, (BATCH, SLOTS), 1)
        visible = slot_ids < seq
        owner = jnp.logical_and(seq >= kv * SLOTS, seq < (kv + 1) * SLOTS)
        tops, totals, news = [], [], []
        for pair in range(HEADS // 2):
            both = []
            for r in (2 * pair, 2 * pair + 1):
                s = jnp.where(visible, s_self[r] * SCALE, MASK_VALUE)
                new = jnp.sum(query[r] * key_new[r // PER], axis=-1, keepdims=True) * SCALE
                new = jnp.where(owner, new, MASK_VALUE)
                top = jnp.maximum(jnp.max(s, axis=-1, keepdims=True), new)
                prob = jnp.where(visible, jnp.exp(s - top), 0.0)
                new_prob = jnp.where(owner, jnp.exp(new - top), 0.0)
                tops.append(top)
                totals.append(jnp.sum(prob, axis=-1, keepdims=True) + new_prob)
                news.append(new_prob)
                both.append(prob)
            p_self[2 * pair * BATCH:(2 * pair + 2) * BATCH, :] = jnp.concatenate(both, axis=0).astype(BF16)
        with jax.named_scope("self_weigh"):
            weigh(vs, p_self)
        outs = [o_v[r] + news[r] * val_new[r // PER] for r in range(HEADS)]
        with jax.named_scope("barrier"):
            pl.semaphore_wait(barrier, len(peers))
        put_partials(0, outs, tops, totals)

    def self_rest(dn, gu):
        start_all(new_copies())
        start_all(copies_up(wg1_h, wu1_h, gu))
        start_all(copies_down(wd1_h, dn))
        start_all(copies_a(wq2_h))
        attn = exchange_partials(0)
        wait_all(copies_o(wo1_h))
        reduce_plane(0, attn, buf_o, 0, 1, lambda h, s: h + s)
        start_all(copies_o(wo2_h))
        mlp(1, 1, 1, gu, dn, copies_up(wg1_h, wu1_h, gu), copies_down(wd1_h, dn))

    up_space = pltpu.VMEM((4, BLK, 2 * FFW), BF16)
    down_space = pltpu.VMEM((4, FFW, BLK), BF16)

    def phase_one(gu):
        pl.run_scoped(functools.partial(self_attention, gu=gu), pltpu.VMEM((4, BLK, 2 * KVW), BF16),
                      pltpu.VMEM((BATCH, GROUPS, SLOTS, HEAD), BF16), pltpu.VMEM((BATCH, GROUPS, SLOTS, HEAD), BF16))
        pl.run_scoped(functools.partial(self_rest, gu=gu), down_space)

    pl.run_scoped(phase_one, up_space)

    visible_tile = seen_here > 0
    row_on = jnp.where(seen > 0, 1.0, 0.0)

    def scope_two(kx, vx):
        caches = [local(kx_h, kx), local(vx_h, vx)]
        gather_all(1, 1, 2, lambda h, s: h + s)
        norm_to_u(2, 2)
        acc = jnp.zeros((BATCH, QW), F32)
        with jax.named_scope("q_cross"):
            wait_all(copies_a(wq2_h))
            for c in range(4):
                acc = acc + dot(u_block(c), buf_a[c])
        query = []
        for r in range(HEADS):
            z = acc[:, r * HEAD:(r + 1) * HEAD]
            z = z * lax.rsqrt(jnp.mean(z * z, axis=-1, keepdims=True) + NORM_EPS) * qn_v[...].astype(F32)
            query.append(bf(z))
        for r in range(HEADS):
            qc_v[r * BATCH:(r + 1) * BATCH, :] = query[r]
        with jax.named_scope("cross_scores"):
            wait_all(caches)
            q = qc_v[...].astype(BF16)
            for b in range(BATCH):
                s = lax.dot_general(q, kx[b * STEP:b * STEP + WIN, :], (((1,), (1,)), ((), ())),
                                    preferred_element_type=F32)
                for r in range(HEADS):
                    s_cross[r, b:b + 1, :] = s[r * BATCH + b:r * BATCH + b + 1, :]
        place = lax.broadcasted_iota(jnp.int32, (BATCH, WIN), 1) - 2 * lax.broadcasted_iota(jnp.int32, (BATCH, WIN), 0)
        inside = jnp.logical_and(place >= 0, place < 2 * TOK)
        tops, totals = [], []
        for pair in range(HEADS // 2):
            both = []
            for r in (2 * pair, 2 * pair + 1):
                mine = jnp.logical_and(inside, lax.rem(place + 16, 2) == r // PER)
                s = jnp.where(mine, s_cross[r] * SCALE, MASK_VALUE)
                top = jnp.max(s, axis=-1, keepdims=True)
                prob = jnp.where(mine, jnp.exp(s - top), 0.0)
                tops.append(jnp.where(visible_tile, top, MASK_VALUE))
                totals.append(jnp.where(visible_tile, jnp.sum(prob, axis=-1, keepdims=True), 0.0))
                both.append(prob)
            p_cross[2 * pair * BATCH:(2 * pair + 2) * BATCH, :] = jnp.concatenate(both, axis=0).astype(BF16)
        with jax.named_scope("cross_weigh"):
            for b in range(BATCH):
                o = dot(p_cross[...], vx[b * STEP:b * STEP + WIN, :])
                for r in range(HEADS):
                    o_v[r, b:b + 1, :] = o[r * BATCH + b:r * BATCH + b + 1, :]
        outs = [jnp.where(visible_tile, o_v[r], 0.0) for r in range(HEADS)]
        put_partials(1, outs, tops, totals)

    pl.run_scoped(scope_two, pltpu.VMEM((ROWS, HEAD), BF16), pltpu.VMEM((ROWS, HEAD), BF16))

    def gate(i):
        return jnp.tanh(jnp.full((BATCH, HEAD), gates_ref[i], F32))[:, 0:1] * row_on

    def scope_three(gu, dn):
        start_all(copies_up(wg2_h, wu2_h, gu))
        start_all(copies_down(wd2_h, dn))
        attn = exchange_partials(1)
        wait_all(copies_o(wo2_h))
        reduce_plane(2, attn, buf_o, 2, 3, lambda h, s: h + gate(0) * s)
        mlp(3, 3, 3, gu, dn, copies_up(wg2_h, wu2_h, gu), copies_down(wd2_h, dn))

    pl.run_scoped(scope_three, up_space, down_space)
    gather_all(3, 3, 4, lambda h, s: h + gate(1) * s)
    with jax.named_scope("put_h"):
        for p in range(8):
            x_v[:, p * PIECE:(p + 1) * PIECE] = hbuf[4, p].astype(BF16)
        put = pltpu.make_async_copy(x_v, h_out, osem.at[2])
        put.start()
        put.wait()
        for copy in new_copies():
            copy.wait()


def put_out(h_in, k_in, v_in, h_out, k_out, v_out):
    h_out[...] = h_in[...]
    for src, dst in ((k_in, k_out), (v_in, v_out)):
        dst[...] = src[...].astype(F32).reshape(BATCH, GROUPS, HEAD).astype(BF16)


def solution(mesh):
    rows_spec = P('dp', None)
    cache_spec = P('dp', 'tp', 'kv', None)
    new_spec = P('dp', 'tp', None)
    col_spec = P(None, 'tp')
    row_spec = P('tp', None)
    vec_spec = P(None)
    in_specs = (rows_spec, cache_spec, cache_spec, P('dp'), cache_spec, cache_spec, rows_spec,
                vec_spec, col_spec, col_spec, col_spec, row_spec, vec_spec, col_spec, col_spec, row_spec,
                vec_spec, col_spec, vec_spec, row_spec, vec_spec, vec_spec, col_spec, col_spec, row_spec)
    out_specs = (rows_spec, new_spec, new_spec)

    def device_step(x, ks_cache, vs_cache, seq_len, kx_cache, vx_cache, tile_vis, attn_norm, wq_self, wk_self, wv_self, wo_self, mlp_norm, wg_self, wu_self, wd_self, xattn_norm, wq_cross, q_norm, wo_cross, cross_gates, xmlp_norm, wg_cross, wu_cross, wd_cross):
        freqs = jnp.asarray(np.tile(rope_freqs(HEAD)[None, :], (BATCH, 1)))
        norms = [gain.reshape(HID // HEAD, HEAD) for gain in (attn_norm, mlp_norm, xattn_norm, xmlp_norm)]
        kx_rows, vx_rows = [cache.transpose(0, 2, 1, 3).reshape(ROWS, HEAD) for cache in (kx_cache, vx_cache)]
        hbm = pl.BlockSpec(memory_space=pl.ANY)
        smem = pl.BlockSpec(memory_space=pltpu.SMEM)
        vmem = pl.BlockSpec(memory_space=pltpu.VMEM)
        piece = (8, BATCH, PIECE)
        scratch = [
            pltpu.VMEM((BATCH, HID), BF16), pltpu.VMEM((2, BATCH, KVW), BF16), pltpu.VMEM((4, HID // HEAD, HEAD), BF16), pltpu.VMEM((1, HEAD), BF16),
            pltpu.VMEM((4, HID // HEAD, HEAD), F32), pltpu.VMEM((3, BATCH, HEAD), F32),
            pltpu.VMEM((4, BLK, BLK), BF16), pltpu.VMEM((4, BLK, BLK), BF16),
            pltpu.VMEM(piece, F32), pltpu.VMEM((HEADS * BATCH, 2 * HEAD), F32), pltpu.VMEM((HEADS * BATCH, HEAD), F32), pltpu.VMEM((HEADS, BATCH, HEAD), F32),
            pltpu.VMEM((HEADS, BATCH, SLOTS), F32), pltpu.VMEM((HEADS * BATCH, SLOTS), BF16),
            pltpu.VMEM((HEADS, BATCH, WIN), F32), pltpu.VMEM((HEADS * BATCH, WIN), BF16),
            pltpu.VMEM((2, 4, BATCH, QW + HEAD), F32),
            pltpu.VMEM((4,) + piece, F32), pltpu.VMEM((4, 4, BATCH, PIECE), F32),
            pltpu.VMEM((4, 4, BATCH, PIECE), F32), pltpu.VMEM((2, 4, BATCH, PIECE), F32),
            pltpu.VMEM((2, 4, BATCH, PIECE), F32), pltpu.VMEM((2, 2) + piece, F32),
            pltpu.VMEM((5,) + piece, F32),
            pltpu.SemaphoreType.DMA((N_LOCAL,)), pltpu.SemaphoreType.DMA((28,)), pltpu.SemaphoreType.DMA((3,)), pltpu.SemaphoreType.DMA((N_REMOTE,)), pltpu.SemaphoreType.DMA((N_REMOTE,)),
        ]
        h, key_new, val_new = pl.pallas_call(
            kernel,
            out_shape=(jax.ShapeDtypeStruct((BATCH, HID), BF16), jax.ShapeDtypeStruct((BATCH, KVW), BF16),
                       jax.ShapeDtypeStruct((BATCH, KVW), BF16)),
            in_specs=[hbm] * 7 + [smem] * 3 + [hbm] * 16,
            out_specs=(hbm, hbm, hbm),
            scratch_shapes=scratch,
            compiler_params=pltpu.CompilerParams(collective_id=0, has_side_effects=True, vmem_limit_bytes=VMEM_LIMIT),
        )(x, *norms, q_norm.reshape(1, HEAD), freqs, cross_gates, seq_len, tile_vis.T, ks_cache, vs_cache, kx_rows, vx_rows,
          wq_self, wk_self, wv_self, wo_self, wg_self, wu_self, wd_self, wq_cross, wo_cross, wg_cross, wu_cross, wd_cross)
        return pl.pallas_call(
            put_out,
            out_shape=(jax.ShapeDtypeStruct((BATCH, HID), BF16), jax.ShapeDtypeStruct((BATCH, GROUPS, HEAD), BF16),
                       jax.ShapeDtypeStruct((BATCH, GROUPS, HEAD), BF16)),
            in_specs=[vmem] * 3, out_specs=(vmem,) * 3)(h, key_new, val_new)

    return jax.shard_map(device_step, mesh=mesh, in_specs=in_specs, out_specs=out_specs, check_vma=False)
```
